32 devices in a mesh: grp: 2 (over x), gx: 16 (over z, y, core).
Axes of the slice: x: 2, y: 2, z: 4, core: 2. Of those that a mesh axis runs over, the one named last changes fastest.
Arguments:
- remaining_states: bfloat16 [128, 16384], P(('grp', 'gx')), parts along dimension 0, may hold values from -6 to 6
- scaling_factor_vector: bfloat16 [16384], replicated, may hold values from 0.25 to 1.75
- probe_projection_matrix: bfloat16 [16384, 8192], P(None, 'gx'), may hold values from -1 to 1
- memory_projection_matrix: bfloat16 [16384, 1024], P('gx'), may hold values from -0.046875 to 0.046875
- final_projection_matrix: bfloat16 [8192, 16384], P('gx'), may hold values from -0.0625 to 0.0625
- memorized_address_tensor: bfloat16 [1024, 128, 512], P(('grp', 'gx')), parts along dimension 0, may hold values from -8 to 8
- memorized_content_tensor: bfloat16 [1024, 128, 512], P(('grp', 'gx')), parts along dimension 0, may hold values from -6 to 6
- retained_sequence_ids: int32 [128], P('grp'), parts along dimension 0, may hold values from 0 to 511, as said below
- occupied_positions: int32 [1024], P(('grp', 'gx')), parts along dimension 0, may hold values from 1 to 128
Outputs:
- result: bfloat16 [128, 16384], P(('grp', 'gx')), parts along dimension 0
The draws below stay inside these ranges and needn't reach their ends.
There are 2 independent parts, one for each index of `grp`. The reference program is written for one: setup_inputs(seed, part) draws one part's arguments, and reference() takes and returns one part's arrays. A program takes and returns all parts, laid end to end along the dimension named above; an argument that names none is the same for every part. Nothing has to cross between parts.
Inputs may be any that keep to these rules, and one draw needn't show every extreme that they name: Distinct batch rows; row r of remaining_states belongs to batch row retained_sequence_ids[r].
All inputs are finite; a program needn't handle non-finite values.
Results may differ from the reference program's by a relative error of at most 0.014.
Values may be sent and summed in bfloat16 or wider, within the bound.
A program may use at most 192 MiB of HBM per device.

```python
import math
import jax
import jax.numpy as jnp
from jax import lax

D = 16384
HEADS = 64
KV = 4
DH = 128
CACHE = 128
ROWS = 64
BATCH = 512


def draw_remaining_states(key, part):
    sampled = jax.random.truncated_normal(key, -6.0, 6.0, (ROWS, D), jnp.float32)
    return sampled.astype(jnp.bfloat16)


def draw_probe_projection_matrix(key, part):
    scale = 1.0 / math.sqrt(D)
    columns_all = HEADS * DH
    sampled = jax.random.truncated_normal(key, -4.0, 4.0, (D, columns_all), jnp.float32) * scale
    return sampled.astype(jnp.bfloat16)


def draw_memorized_address_tensor(key, part):
    sampled = jax.random.truncated_normal(key, -6.0, 6.0, (BATCH, CACHE, KV * DH), jnp.float32)
    return sampled.astype(jnp.bfloat16)


def draw_retained_sequence_ids(key, part):
    shuffled = jax.random.permutation(key, BATCH)
    return shuffled[:ROWS].astype(jnp.int32)


def place_ends(values, rng, least, top_value):
    longest = values.shape.index(max(values.shape))
    spots = []
    for shift in (0, 1):
        where = [jax.random.randint(jax.random.fold_in(rng, axis), (), 0, length) for axis, length in enumerate(values.shape)]
        where[longest] = (where[longest] + shift) % values.shape[longest]
        spots.append(tuple(where))
    return values.at[spots[0]].set(least).at[spots[1]].set(top_value)


def shard_levels(rng, extent, split, low, top_value):
    def one(dim, parts):
        draws = jax.random.uniform(jax.random.fold_in(jax.random.fold_in(rng, 6), dim), (parts,), jnp.float32, low / len(split), top_value / len(split))
        return jnp.repeat(jnp.exp(draws), extent[dim] // parts).reshape((-1,) + (1,) * (len(extent) - dim - 1))

    loudness = one(*split[0])
    for cut in split[1:]:
        loudness = loudness * one(*cut)
    return loudness


def centred(own_key, extent, deviation, limit, split=(), held_as=jnp.bfloat16):
    drawn = jax.random.normal(own_key, extent, jnp.float32) * deviation
    if len(split) > 0:
        drawn = shard_levels(own_key, extent, split, -0.22, 0.18) * drawn
    return jnp.clip(drawn, min=-limit, max=limit).astype(held_as)


def setup_inputs(seed: int = 0, part: int = 0) -> dict:
    seeds = jax.random.split(jax.random.key(seed), 10)
    own_keys = jax.random.split(jax.random.fold_in(seeds[9], part), 10)
    remaining_states = draw_remaining_states(jax.random.fold_in(jax.random.fold_in(seeds[9], part), 71), part)
    scaling_factor_vector = jnp.clip(1.0 + 0.15 * jax.random.normal(seeds[1], (D,), jnp.float32), 0.25, 1.75).astype(jnp.bfloat16)
    probe_projection_matrix = draw_probe_projection_matrix(jax.random.fold_in(seeds[9], 71), part)
    memory_projection_matrix = centred(seeds[3], (D, 2 * KV * DH), D ** -0.5, 0.046875, ((0, 16),))
    final_projection_matrix = centred(seeds[4], (HEADS * DH, D), (HEADS * DH) ** -0.5, 0.0625, ((0, 16),))
    memorized_address_tensor = draw_memorized_address_tensor(jax.random.fold_in(jax.random.fold_in(seeds[9], part), 71), part)
    memorized_content_tensor = centred(own_keys[6], (BATCH, CACHE, KV * DH), 1.0, 6.0, ((0, 16),))
    retained_sequence_ids = draw_retained_sequence_ids(jax.random.fold_in(jax.random.fold_in(seeds[9], part), 71), part)
    occupied_positions = place_ends(jax.random.randint(own_keys[8], (BATCH,), 1, CACHE + 1), jax.random.fold_in(own_keys[8], 1), 1, CACHE).astype(jnp.int32)
    return dict(remaining_states=remaining_states, scaling_factor_vector=scaling_factor_vector, probe_projection_matrix=probe_projection_matrix, memory_projection_matrix=memory_projection_matrix, final_projection_matrix=final_projection_matrix, memorized_address_tensor=memorized_address_tensor, memorized_content_tensor=memorized_content_tensor, retained_sequence_ids=retained_sequence_ids, occupied_positions=occupied_positions)


epsilon = 1e-05

def attend_rows(probe_vectors, new_kv, keys, values, retained_fill_counts):
    slots = probe_vectors.shape[0]
    query_heads = probe_vectors.astype(jnp.float32).reshape(slots, KV, HEADS // KV, DH)
    key_heads = keys.astype(jnp.float32).reshape(slots, CACHE, KV, DH)
    value_heads = values.astype(jnp.float32).reshape(slots, CACHE, KV, DH)
    inverse = 1.0 / jnp.sqrt(jnp.float32(DH))
    scores = jnp.einsum('skgd,sjkd->skgj', query_heads, key_heads) * inverse
    visible = (jnp.arange(CACHE, dtype=jnp.int32)[None, :] < retained_fill_counts[:, None])[:, None, None, :]
    scores = jnp.where(visible, scores, jnp.float32(-1e+30))
    new_keys = new_kv[:, :KV * DH].astype(jnp.float32).reshape(slots, KV, 1, DH)
    new_values = new_kv[:, KV * DH:].astype(jnp.float32).reshape(slots, KV, 1, DH)
    own_score = lax.optimization_barrier(jnp.sum(query_heads * new_keys, axis=-1)) * inverse
    highest = jnp.maximum(lax.optimization_barrier(jnp.max(scores, axis=-1)), own_score)
    expo_cache = jnp.where(visible, jnp.exp(scores - highest[..., None]), jnp.float32(0.0))
    expo_new = jnp.exp(own_score - highest)
    denominator = lax.optimization_barrier(jnp.sum(expo_cache, axis=-1)) + expo_new
    weights = (expo_cache / denominator[..., None]).astype(jnp.bfloat16)
    weight_new = (expo_new / denominator).astype(jnp.bfloat16)
    summed = jnp.einsum('skgj,sjkd->skgd', weights.astype(jnp.float32), value_heads)
    summed = summed + weight_new.astype(jnp.float32)[..., None] * new_values
    return summed.reshape(slots, HEADS * DH).astype(jnp.bfloat16)

def reference(remaining_states, scaling_factor_vector, probe_projection_matrix, memory_projection_matrix, final_projection_matrix, memorized_address_tensor, memorized_content_tensor, retained_sequence_ids, occupied_positions):
    values = remaining_states.astype(jnp.float32)
    inverse = lax.rsqrt(lax.optimization_barrier(jnp.mean(values * values, axis=1, keepdims=True)) + epsilon)
    normed = (values * inverse * scaling_factor_vector.astype(jnp.float32)).astype(jnp.bfloat16)
    probe_vectors = jnp.dot(normed, probe_projection_matrix, preferred_element_type=jnp.float32).astype(jnp.bfloat16)
    new_kv = jnp.dot(normed, memory_projection_matrix, preferred_element_type=jnp.float32).astype(jnp.bfloat16)
    retained_address_tensor = memorized_address_tensor[retained_sequence_ids]
    retained_content_tensor = memorized_content_tensor[retained_sequence_ids]
    retained_fill_counts = occupied_positions[retained_sequence_ids]
    attended = attend_rows(probe_vectors, new_kv, retained_address_tensor, retained_content_tensor, retained_fill_counts)
    projected = jnp.dot(attended, final_projection_matrix, preferred_element_type=jnp.float32)
    return (values + projected).astype(jnp.bfloat16)
```

```python
import functools
import jax
import jax.numpy as jnp
from jax import lax
from jax.experimental import pallas as pl
from jax.experimental.pallas import tpu as pltpu
from jax.sharding import PartitionSpec as P

HEADS = 64
KV = 4
DH = 128
CACHE = 128

epsilon = 1e-05
F32 = jnp.float32
BF16 = jnp.bfloat16


def place(n):
    me = lax.axis_index("gx")
    return me, me // 4, (me // 2) % 2, me % 2, n // 4


def dev(z, y, c):
    return (z * 2 + y) * 2 + c


def enter(n):
    me = lax.axis_index("gx")
    barrier = pltpu.get_barrier_semaphore()
    for k in range(1, n):
        pl.semaphore_signal(
            barrier,
            inc=1,
            device_id={"gx": lax.rem(me + k, n)},
            device_id_type=pl.DeviceIdType.MESH,
        )
    pl.semaphore_wait(barrier, n - 1)


def remote(src, dst, send, recv, target):
    return pltpu.make_async_remote_copy(
        src_ref=src,
        dst_ref=dst,
        send_sem=send,
        recv_sem=recv,
        device_id={"gx": target},
        device_id_type=pl.DeviceIdType.MESH,
    )


class Gather:
    def __init__(self, n, g, send, recv):
        self.n, self.g, self.send, self.recv = n, g, send, recv
        self.me, self.z, self.y, self.c, self.Z = place(n)
        self.other_y = dev(self.z, 1 - self.y, self.c)
        self.other_c = dev(self.z, self.y, 1 - self.c)

    def copy(self, ch, block, kind, target):
        return remote(
            self.g.at[ch, block],
            self.g.at[ch, block],
            self.send.at[kind, ch, block],
            self.recv.at[ch, block],
            target,
        )

    def arrived(self, ch, block):
        self.copy(ch, block, 3, self.other_c).wait_recv()

    def fan(self, ch, sz):
        block = dev(sz, self.y, self.c)
        z, Z = self.z, self.Z

        @pl.when((sz <= z) & (z < Z - 1))
        def _():
            self.copy(ch, block, 0, self.me + 4).start()

        @pl.when((sz >= z) & (z > 0))
        def _():
            self.copy(ch, block, 1, self.me - 4).start()

        self.copy(ch, block, 2, self.other_y).start()
        self.copy(ch, block, 3, self.other_c).start()

    def both(self, t, f):
        z, Z = self.z, self.Z
        if t == 0:
            f(z)
            return

        @pl.when(z >= t)
        def _():
            f(z - t)

        @pl.when(z + t < Z)
        def _():
            f(z + t)

    def own(self, ch):
        self.fan(ch, self.z)

    def line(self, ch, t):
        def f(sz):
            self.arrived(ch, dev(sz, self.y, self.c))
            self.fan(ch, sz)

        self.both(t, f)

    def across(self, ch, t):
        def f(sz):
            block = dev(sz, 1 - self.y, self.c)
            self.arrived(ch, block)
            self.copy(ch, block, 3, self.other_c).start()

        self.both(t, f)

    def rest(self, ch):
        for sz in range(self.Z):
            for y in range(2):
                self.arrived(ch, dev(sz, y, 1 - self.c))

    def drain(self, ch):
        z, Z = self.z, self.Z
        for sz in range(Z):
            block = dev(sz, self.y, self.c)

            @pl.when((sz <= z) & (z < Z - 1))
            def _():
                self.copy(ch, block, 0, self.other_c).wait_send()

            @pl.when((sz >= z) & (z > 0))
            def _():
                self.copy(ch, block, 1, self.other_c).wait_send()

            self.copy(ch, block, 2, self.other_y).wait_send()
            self.copy(ch, block, 3, self.other_c).wait_send()
            self.copy(ch, dev(sz, 1 - self.y, self.c), 3, self.other_c).wait_send()


def first_kernel(
    n, NC, x_ref, gain_ref, wq_hbm, wkv_hbm, q_ref, kv_ref,
    g, xfull, acc, wq, wkv, kvs, kvr,
    wq_sem, wkv_sem, g_send, g_recv, q_send, q_recv, kv_send, kv_recv, ks, kr,
):
    me, z, y, c, Z = place(n)
    rl, D = x_ref.shape
    R = n * rl
    CW = D // NC
    weight_copies = []
    for ch in range(NC):
        rows = pl.ds(ch * CW, CW)
        cp = pltpu.make_async_copy(wq_hbm.at[rows], wq.at[rows], wq_sem.at[ch])
        cp.start()
        weight_copies.append(cp)
    kv_copy = pltpu.make_async_copy(wkv_hbm, wkv, wkv_sem)
    kv_copy.start()

    square = jnp.zeros((rl, 1), F32)
    for ch in range(NC):
        v = x_ref[:, ch * CW : (ch + 1) * CW].astype(F32)
        square = square + jnp.sum(v * v, axis=1, keepdims=True)
    inverse = lax.rsqrt(square / D + epsilon)
    for ch in range(NC):
        cols = slice(ch * CW, (ch + 1) * CW)
        v = x_ref[:, cols].astype(F32) * inverse * gain_ref[:, cols].astype(F32)
        g[ch, me] = v.astype(BF16)

    enter(n)
    ag = Gather(n, g, g_send, g_recv)
    for ch in range(NC):
        ag.own(ch)

    width = wkv.shape[0]

    def load(ch):
        step = min(512, CW)

        def body(i, carry):
            off = pl.multiple_of(i * step, step)
            pieces = [g[ch, b, :, pl.ds(off, step)].astype(F32) for b in range(n)]
            full = jnp.concatenate(pieces, axis=0).astype(BF16)
            xfull[:, pl.ds(pl.multiple_of(ch * CW + i * step, step), step)] = full
            return carry

        lax.fori_loop(0, CW // step, body, 0)

    def multiply(ch):
        weight_copies[ch].wait()
        step = min(1024, CW)

        def body(i, carry):
            rows = pl.ds(pl.multiple_of(ch * CW + i * step, step), step)
            acc[...] += jnp.dot(xfull[:, rows], wq[rows, :], preferred_element_type=F32)
            return carry

        lax.fori_loop(0, CW // step, body, 0)

    acc[...] = jnp.zeros_like(acc)
    LAG = 2
    for w in range(1, NC + Z + LAG + 1):
        for ch in range(NC):
            t = w - ch
            if 1 <= t < Z:
                ag.line(ch, t)
            ty = t - LAG
            if 0 <= ty < Z:
                ag.across(ch, ty)
            if ty == Z:
                ag.rest(ch)
                load(ch)
                if ch < NC - 1:
                    multiply(ch)

    kv_copy.wait()
    part = jnp.dot(
        xfull[:, pl.ds(pl.multiple_of(me * width, width), width)],
        wkv[...],
        preferred_element_type=F32,
    )
    for p in range(n):
        kvs[p] = part[p * rl : (p + 1) * rl].astype(BF16)
    for k in range(1, n):
        p = lax.rem(me + k, n)
        remote(kvs.at[p], kvr.at[me], ks.at[p], kr.at[me], p).start()
    multiply(NC - 1)

    q_ref[0, me] = acc[...].astype(BF16)
    qg = Gather(n, q_ref, q_send, q_recv)
    qg.own(0)
    total = kvs[me].astype(F32)
    for k in range(1, n):
        p = lax.rem(me + k, n)
        remote(kvs.at[p], kvr.at[p], ks.at[p], kr.at[p], p).wait_recv()
        total = total + kvr[p].astype(F32)
    kv_ref[0, me] = total.astype(BF16)
    kg = Gather(n, kv_ref, kv_send, kv_recv)
    kg.own(0)
    for w in range(1, Z + LAG + 1):
        if w < Z:
            qg.line(0, w)
            kg.line(0, w)
        if 0 <= w - LAG < Z:
            qg.across(0, w - LAG)
            kg.across(0, w - LAG)
    qg.rest(0)
    kg.rest(0)
    for ch in range(NC):
        ag.drain(ch)
    qg.drain(0)
    kg.drain(0)
    for k in range(1, n):
        p = lax.rem(me + k, n)
        remote(kvs.at[p], kvr.at[me], ks.at[p], kr.at[me], p).wait_send()


def project_in(n, x, gain, wq, wkv):
    rl, D = x.shape
    NC = 4
    CW = D // NC
    cols = wq.shape[1]
    wide = wkv.shape[1]
    R = n * rl
    vm = pl.BlockSpec(memory_space=pltpu.VMEM)
    hbm = pl.BlockSpec(memory_space=pl.ANY)
    dma = pltpu.SemaphoreType.DMA
    q, kv = pl.pallas_call(
        functools.partial(first_kernel, n, NC),
        out_shape=(
            jax.ShapeDtypeStruct((1, n, R, cols), BF16),
            jax.ShapeDtypeStruct((1, n, rl, wide), BF16),
        ),
        in_specs=[vm, vm, hbm, hbm],
        out_specs=(vm, vm),
        scratch_shapes=[
            pltpu.VMEM((NC, n, rl, CW), BF16),
            pltpu.VMEM((R, D), BF16),
            pltpu.VMEM((R, cols), F32),
            pltpu.VMEM((D, cols), BF16),
            pltpu.VMEM(wkv.shape, BF16),
            pltpu.VMEM((n, rl, wide), BF16),
            pltpu.VMEM((n, rl, wide), BF16),
            dma((NC,)),
            dma,
            dma((4, NC, n)),
            dma((NC, n)),
            dma((4, 1, n)),
            dma((1, n)),
            dma((4, 1, n)),
            dma((1, n)),
            dma((n,)),
            dma((n,)),
        ],
        compiler_params=pltpu.CompilerParams(
            collective_id=0, has_side_effects=True, vmem_limit_bytes=60 * 1024 * 1024
        ),
        name="project_in",
    )(x, gain.reshape(1, D), wq, wkv)
    return q[0], kv[0]


def second_kernel(
    n, NF, att_ref, ret_ref, x_ref, wo_hbm, out_ref,
    wo, ra, rows, pf, cs, cr, s1, ys, yr, zf, zs, zr,
    wo_sem, a_send, a_recv, c_send, c_recv, y_send, y_recv, z_send, z_recv,
):
    me, z, y, c, Z = place(n)
    rl, D = x_ref.shape
    R = n * rl
    NW = D // NF
    H, Q = R // 2, R // 4
    other_y, other_c = dev(z, 1 - y, c), dev(z, y, 1 - c)
    weight_copies = []
    for ch in range(NF):
        cols = pl.ds(ch * NW, NW)
        cp = pltpu.make_async_copy(wo_hbm.at[:, cols], wo.at[:, cols], wo_sem.at[ch])
        cp.start()
        weight_copies.append(cp)
    enter(n)
    for k in range(1, n):
        p = lax.rem(me + k, n)
        remote(att_ref.at[p], ra.at[me], a_send.at[p], a_recv.at[me], p).start()
    ra[me] = att_ref[me]
    for k in range(1, n):
        p = lax.rem(me + k, n)
        remote(att_ref.at[p], ra.at[p], a_send.at[p], a_recv.at[p], p).wait_recv()
    slots = ra.shape[0] * ra.shape[1]
    rows[...] = jnp.dot(
        ret_ref[...], ra[...].reshape(slots, ra.shape[2]), preferred_element_type=F32
    ).astype(BF16)

    def core_copy(ch):
        return remote(cs.at[ch], cr.at[ch], c_send.at[ch], c_recv.at[ch], other_c)

    def y_copy(ch):
        return remote(ys.at[ch], yr.at[ch], y_send.at[ch], y_recv.at[ch], other_y)

    def z_copy(ch, zz):
        return remote(
            zs.at[ch, zz], zr.at[ch, z], z_send.at[ch, zz], z_recv.at[ch, z], dev(zz, y, c)
        )

    def z_wait(ch, zz):
        remote(
            zs.at[ch, zz], zr.at[ch, zz], z_send.at[ch, zz], z_recv.at[ch, zz], dev(zz, y, c)
        ).wait_recv()

    def matmul(ch):
        weight_copies[ch].wait()
        step = min(1024, NW)
        for i in range(NW // step):
            off = ch * NW + i * step
            pf[ch, :, i * step : (i + 1) * step] = jnp.dot(
                rows[...], wo[:, off : off + step], preferred_element_type=F32
            )
        cs[ch] = pf[ch, pl.ds(pl.multiple_of((1 - c) * H, H), H), :].astype(BF16)
        core_copy(ch).start()

    def core_step(ch):
        core_copy(ch).wait_recv()
        s1[ch] = pf[ch, pl.ds(pl.multiple_of(c * H, H), H), :] + cr[ch].astype(F32)
        ys[ch] = s1[ch, pl.ds(pl.multiple_of((1 - y) * Q, Q), Q), :].astype(BF16)
        y_copy(ch).start()

    def y_step(ch):
        y_copy(ch).wait_recv()
        s = s1[ch, pl.ds(pl.multiple_of(y * Q, Q), Q), :] + yr[ch].astype(F32)
        for zz in range(Z):
            zf[ch, zz] = s[zz * rl : (zz + 1) * rl]
            zs[ch, zz] = s[zz * rl : (zz + 1) * rl].astype(BF16)
        for k in range(1, Z):
            z_copy(ch, lax.rem(z + k, Z)).start()

    def z_step(ch):
        cols = slice(ch * NW, (ch + 1) * NW)
        total = x_ref[:, cols].astype(F32) + zf[ch, z]
        for k in range(1, Z):
            zz = lax.rem(z + k, Z)
            z_wait(ch, zz)
            total = total + zr[ch, zz].astype(F32)
        out_ref[:, cols] = total.astype(BF16)

    for i in range(NF + 5):
        if i < NF:
            matmul(i)
        if 0 <= i - 1 < NF:
            core_step(i - 1)
        if 0 <= i - 3 < NF:
            y_step(i - 3)
        if 0 <= i - 5 < NF:
            z_step(i - 5)
    for k in range(1, n):
        p = lax.rem(me + k, n)
        remote(att_ref.at[p], ra.at[me], a_send.at[p], a_recv.at[me], p).wait_send()
    for ch in range(NF):
        core_copy(ch).wait_send()
        y_copy(ch).wait_send()
        for k in range(1, Z):
            z_copy(ch, lax.rem(z + k, Z)).wait_send()


def project_out(n, att, ret, x, wo):
    rl, D = x.shape
    NF = 8
    NW = D // NF
    R = n * rl
    Z = n // 4
    vm = pl.BlockSpec(memory_space=pltpu.VMEM)
    hbm = pl.BlockSpec(memory_space=pl.ANY)
    dma = pltpu.SemaphoreType.DMA
    return pl.pallas_call(
        functools.partial(second_kernel, n, NF),
        out_shape=jax.ShapeDtypeStruct((rl, D), BF16),
        in_specs=[vm, vm, vm, hbm],
        out_specs=vm,
        scratch_shapes=[
            pltpu.VMEM(wo.shape, BF16),
            pltpu.VMEM(att.shape, BF16),
            pltpu.VMEM((R, wo.shape[0]), BF16),
            pltpu.VMEM((NF, R, NW), F32),
            pltpu.VMEM((NF, R // 2, NW), BF16),
            pltpu.VMEM((NF, R // 2, NW), BF16),
            pltpu.VMEM((NF, R // 2, NW), F32),
            pltpu.VMEM((NF, R // 4, NW), BF16),
            pltpu.VMEM((NF, R // 4, NW), BF16),
            pltpu.VMEM((NF, Z, rl, NW), F32),
            pltpu.VMEM((NF, Z, rl, NW), BF16),
            pltpu.VMEM((NF, Z, rl, NW), BF16),
            dma((NF,)),
            dma((n,)),
            dma((n,)),
            dma((NF,)),
            dma((NF,)),
            dma((NF,)),
            dma((NF,)),
            dma((NF, Z)),
            dma((NF, Z)),
        ],
        compiler_params=pltpu.CompilerParams(
            collective_id=1, has_side_effects=True, vmem_limit_bytes=60 * 1024 * 1024
        ),
        name="project_out",
    )(att, ret, x, wo)


def attend_slots(probe_vectors, new_kv, keys, values, slot_lengths):
    slots = probe_vectors.shape[0]
    query_heads = probe_vectors.reshape(slots, KV, HEADS // KV, DH)
    key_heads = keys.reshape(slots, CACHE, KV, DH)
    value_heads = values.reshape(slots, CACHE, KV, DH)
    inverse = 1.0 / jnp.sqrt(jnp.float32(DH))
    scores = (
        jnp.einsum("skgd,sjkd->skgj", query_heads, key_heads, preferred_element_type=jnp.float32)
        * inverse
    )
    visible = (jnp.arange(CACHE, dtype=jnp.int32)[None, :] < slot_lengths[:, None])[
        :, None, None, :
    ]
    scores = jnp.where(visible, scores, jnp.float32(-1e30))
    new_keys = new_kv[:, : KV * DH].astype(jnp.float32).reshape(slots, KV, 1, DH)
    new_values = new_kv[:, KV * DH :].astype(jnp.float32).reshape(slots, KV, 1, DH)
    own_score = jnp.sum(query_heads.astype(jnp.float32) * new_keys, axis=-1) * inverse
    highest = jnp.maximum(jnp.max(scores, axis=-1), own_score)
    expo_cache = jnp.where(visible, jnp.exp(scores - highest[..., None]), jnp.float32(0.0))
    expo_new = jnp.exp(own_score - highest)
    denominator = jnp.sum(expo_cache, axis=-1) + expo_new
    weights = (expo_cache / denominator[..., None]).astype(jnp.bfloat16)
    weight_new = (expo_new / denominator).astype(jnp.bfloat16)
    summed = jnp.einsum("skgj,sjkd->skgd", weights, value_heads, preferred_element_type=jnp.float32)
    summed = summed + weight_new.astype(jnp.float32)[..., None] * new_values
    return summed.reshape(slots, HEADS * DH).astype(jnp.bfloat16)


def local(
    remaining_states,
    scaling_factor_vector,
    probe_projection_matrix,
    memory_projection_matrix,
    final_projection_matrix,
    memorized_address_tensor,
    memorized_content_tensor,
    retained_sequence_ids,
    occupied_positions,
):
    n = lax.axis_size("gx")
    me = lax.axis_index("gx")
    slots = memorized_address_tensor.shape[0]
    rl = remaining_states.shape[0]
    R = n * rl
    q_all, kv_all = project_in(
        n,
        remaining_states,
        scaling_factor_vector,
        probe_projection_matrix,
        memory_projection_matrix,
    )
    mine = (
        retained_sequence_ids[None, :]
        == (me * slots + jnp.arange(slots, dtype=jnp.int32))[:, None]
    ).astype(BF16)
    owner_queries = jnp.einsum(
        "sr,drc->sdc", mine, q_all, preferred_element_type=F32
    ).astype(BF16).reshape(slots, -1)
    new_kv = jnp.dot(
        mine, kv_all.reshape(R, -1), preferred_element_type=F32
    ).astype(BF16)
    attended = attend_slots(
        owner_queries,
        new_kv,
        memorized_address_tensor,
        memorized_content_tensor,
        occupied_positions,
    )
    att = jnp.transpose(attended.reshape(slots, n, -1), (1, 0, 2))
    ids = jnp.transpose(
        retained_sequence_ids.reshape(n // 4, 2, 2, rl), (2, 1, 0, 3)
    ).reshape(R)
    ret = (ids[:, None] == jnp.arange(n * slots, dtype=jnp.int32)[None, :]).astype(BF16)
    return project_out(n, att, ret, remaining_states, final_projection_matrix)


def solution(mesh):
    placed = (
        P(("grp", "gx"), None),
        P(),
        P(None, "gx"),
        P("gx", None),
        P("gx", None),
        P(("grp", "gx"), None, None),
        P(("grp", "gx"), None, None),
        P("grp"),
        P(("grp", "gx")),
    )
    return jax.shard_map(
        local, mesh=mesh, in_specs=placed, out_specs=P(("grp", "gx"), None), check_vma=False
    )
```

```python
import functools
import jax
import jax.numpy as jnp
from jax import lax
from jax.experimental import pallas as pl
from jax.experimental.pallas import tpu as pltpu
from jax.sharding import PartitionSpec as P

HEADS = 64
KV = 4
DH = 128
CACHE = 128

epsilon = 1e-05
F32 = jnp.float32
BF16 = jnp.bfloat16


def place(n):
    me = lax.axis_index("gx")
    return me, me // 4, (me // 2) % 2, me % 2, n // 4


def dev(z, y, c):
    return (z * 2 + y) * 2 + c


def enter(n):
    me = lax.axis_index("gx")
    barrier = pltpu.get_barrier_semaphore()
    for k in range(1, n):
        pl.semaphore_signal(
            barrier,
            inc=1,
            device_id={"gx": lax.rem(me + k, n)},
            device_id_type=pl.DeviceIdType.MESH,
        )
    pl.semaphore_wait(barrier, n - 1)


def remote(src, dst, send, recv, target):
    return pltpu.make_async_remote_copy(
        src_ref=src,
        dst_ref=dst,
        send_sem=send,
        recv_sem=recv,
        device_id={"gx": target},
        device_id_type=pl.DeviceIdType.MESH,
    )


class Gather:
    def __init__(self, n, g, send, recv):
        self.n, self.g, self.send, self.recv = n, g, send, recv
        self.me, self.z, self.y, self.c, self.Z = place(n)
        self.other_y = dev(self.z, 1 - self.y, self.c)
        self.other_c = dev(self.z, self.y, 1 - self.c)

    def copy(self, ch, block, kind, target):
        return remote(
            self.g.at[ch, block],
            self.g.at[ch, block],
            self.send.at[kind, ch, block],
            self.recv.at[ch, block],
            target,
        )

    def arrived(self, ch, block):
        self.copy(ch, block, 3, self.other_c).wait_recv()

    def fan(self, ch, sz):
        block = dev(sz, self.y, self.c)
        z, Z = self.z, self.Z

        @pl.when((sz <= z) & (z < Z - 1))
        def _():
            self.copy(ch, block, 0, self.me + 4).start()

        @pl.when((sz >= z) & (z > 0))
        def _():
            self.copy(ch, block, 1, self.me - 4).start()

        self.copy(ch, block, 2, self.other_y).start()
        self.copy(ch, block, 3, self.other_c).start()

    def both(self, t, f):
        z, Z = self.z, self.Z
        if t == 0:
            f(z)
            return

        @pl.when(z >= t)
        def _():
            f(z - t)

        @pl.when(z + t < Z)
        def _():
            f(z + t)

    def own(self, ch):
        self.fan(ch, self.z)

    def line(self, ch, t):
        def f(sz):
            self.arrived(ch, dev(sz, self.y, self.c))
            self.fan(ch, sz)

        self.both(t, f)

    def across(self, ch, t):
        def f(sz):
            block = dev(sz, 1 - self.y, self.c)
            self.arrived(ch, block)
            self.copy(ch, block, 3, self.other_c).start()

        self.both(t, f)

    def rest(self, ch):
        for sz in range(self.Z):
            for y in range(2):
                self.arrived(ch, dev(sz, y, 1 - self.c))

    def drain(self, ch):
        z, Z = self.z, self.Z
        for sz in range(Z):
            block = dev(sz, self.y, self.c)

            @pl.when((sz <= z) & (z < Z - 1))
            def _():
                self.copy(ch, block, 0, self.other_c).wait_send()

            @pl.when((sz >= z) & (z > 0))
            def _():
                self.copy(ch, block, 1, self.other_c).wait_send()

            self.copy(ch, block, 2, self.other_y).wait_send()
            self.copy(ch, block, 3, self.other_c).wait_send()
            self.copy(ch, dev(sz, 1 - self.y, self.c), 3, self.other_c).wait_send()


def first_kernel(
    n, NC, x_ref, gain_ref, wq_hbm, wkv_hbm, q_ref, kv_ref,
    g, xfull, acc, wq, wkv, kvs, kvr,
    wq_sem, wkv_sem, g_send, g_recv, q_send, q_recv, kv_send, kv_recv, ks, kr,
):
    me, z, y, c, Z = place(n)
    rl, D = x_ref.shape
    R = n * rl
    CW = D // NC
    weight_copies = []
    for ch in range(NC):
        rows = pl.ds(ch * CW, CW)
        cp = pltpu.make_async_copy(wq_hbm.at[rows], wq.at[rows], wq_sem.at[ch])
        cp.start()
        weight_copies.append(cp)
    kv_copy = pltpu.make_async_copy(wkv_hbm, wkv, wkv_sem)
    kv_copy.start()

    square = jnp.zeros((rl, 1), F32)
    for ch in range(NC):
        v = x_ref[:, ch * CW : (ch + 1) * CW].astype(F32)
        square = square + jnp.sum(v * v, axis=1, keepdims=True)
    inverse = lax.rsqrt(square / D + epsilon)
    for ch in range(NC):
        cols = slice(ch * CW, (ch + 1) * CW)
        v = x_ref[:, cols].astype(F32) * inverse * gain_ref[:, cols].astype(F32)
        g[ch, me] = v.astype(BF16)

    enter(n)
    ag = Gather(n, g, g_send, g_recv)
    for ch in range(NC):
        ag.own(ch)

    width = wkv.shape[0]

    def load(ch):
        step = min(512, CW)

        def body(i, carry):
            off = pl.multiple_of(i * step, step)
            pieces = [g[ch, b, :, pl.ds(off, step)].astype(F32) for b in range(n)]
            full = jnp.concatenate(pieces, axis=0).astype(BF16)
            xfull[:, pl.ds(pl.multiple_of(ch * CW + i * step, step), step)] = full
            return carry

        lax.fori_loop(0, CW // step, body, 0)

    def multiply(ch):
        weight_copies[ch].wait()
        step = min(1024, CW)

        def body(i, carry):
            rows = pl.ds(pl.multiple_of(ch * CW + i * step, step), step)
            acc[...] += jnp.dot(xfull[:, rows], wq[rows, :], preferred_element_type=F32)
            return carry

        lax.fori_loop(0, CW // step, body, 0)

    acc[...] = jnp.zeros_like(acc)
    LAG = 2
    for w in range(1, NC + Z + LAG + 1):
        for ch in range(NC):
            t = w - ch
            if 1 <= t < Z:
                ag.line(ch, t)
            ty = t - LAG
            if 0 <= ty < Z:
                ag.across(ch, ty)
            if ty == Z:
                ag.rest(ch)
                load(ch)
                if ch < NC - 1:
                    multiply(ch)

    kv_copy.wait()
    part = jnp.dot(
        xfull[:, pl.ds(pl.multiple_of(me * width, width), width)],
        wkv[...],
        preferred_element_type=F32,
    )
    for p in range(n):
        kvs[p] = part[p * rl : (p + 1) * rl].astype(BF16)
    for k in range(1, n):
        p = lax.rem(me + k, n)
        remote(kvs.at[p], kvr.at[me], ks.at[p], kr.at[me], p).start()
    multiply(NC - 1)

    q_ref[0, me] = acc[...].astype(BF16)
    qg = Gather(n, q_ref, q_send, q_recv)
    qg.own(0)
    total = kvs[me].astype(F32)
    for k in range(1, n):
        p = lax.rem(me + k, n)
        remote(kvs.at[p], kvr.at[p], ks.at[p], kr.at[p], p).wait_recv()
        total = total + kvr[p].astype(F32)
    kv_ref[0, me] = total.astype(BF16)
    kg = Gather(n, kv_ref, kv_send, kv_recv)
    kg.own(0)
    for w in range(1, Z + LAG + 1):
        if w < Z:
            qg.line(0, w)
            kg.line(0, w)
        if 0 <= w - LAG < Z:
            qg.across(0, w - LAG)
            kg.across(0, w - LAG)
    qg.rest(0)
    kg.rest(0)
    for ch in range(NC):
        ag.drain(ch)
    qg.drain(0)
    kg.drain(0)
    for k in range(1, n):
        p = lax.rem(me + k, n)
        remote(kvs.at[p], kvr.at[me], ks.at[p], kr.at[me], p).wait_send()


def project_in(n, x, gain, wq, wkv):
    rl, D = x.shape
    NC = 2
    CW = D // NC
    cols = wq.shape[1]
    wide = wkv.shape[1]
    R = n * rl
    vm = pl.BlockSpec(memory_space=pltpu.VMEM)
    hbm = pl.BlockSpec(memory_space=pl.ANY)
    dma = pltpu.SemaphoreType.DMA
    q, kv = pl.pallas_call(
        functools.partial(first_kernel, n, NC),
        out_shape=(
            jax.ShapeDtypeStruct((1, n, R, cols), BF16),
            jax.ShapeDtypeStruct((1, n, rl, wide), BF16),
        ),
        in_specs=[vm, vm, hbm, hbm],
        out_specs=(vm, vm),
        scratch_shapes=[
            pltpu.VMEM((NC, n, rl, CW), BF16),
            pltpu.VMEM((R, D), BF16),
            pltpu.VMEM((R, cols), F32),
            pltpu.VMEM((D, cols), BF16),
            pltpu.VMEM(wkv.shape, BF16),
            pltpu.VMEM((n, rl, wide), BF16),
            pltpu.VMEM((n, rl, wide), BF16),
            dma((NC,)),
            dma,
            dma((4, NC, n)),
            dma((NC, n)),
            dma((4, 1, n)),
            dma((1, n)),
            dma((4, 1, n)),
            dma((1, n)),
            dma((n,)),
            dma((n,)),
        ],
        compiler_params=pltpu.CompilerParams(
            collective_id=0, has_side_effects=True, vmem_limit_bytes=60 * 1024 * 1024
        ),
        name="project_in",
    )(x, gain.reshape(1, D), wq, wkv)
    return q[0], kv[0]


def second_kernel(
    n, NF, att_ref, ret_ref, x_ref, wo_hbm, out_ref,
    wo, ra, rows, pf, cs, cr, s1, ys, yr, zf, zs, zr,
    wo_sem, a_send, a_recv, c_send, c_recv, y_send, y_recv, z_send, z_recv,
):
    me, z, y, c, Z = place(n)
    rl, D = x_ref.shape
    R = n * rl
    NW = D // NF
    H, Q = R // 2, R // 4
    other_y, other_c = dev(z, 1 - y, c), dev(z, y, 1 - c)
    weight_copies = []
    for ch in range(NF):
        cols = pl.ds(ch * NW, NW)
        cp = pltpu.make_async_copy(wo_hbm.at[:, cols], wo.at[:, cols], wo_sem.at[ch])
        cp.start()
        weight_copies.append(cp)
    enter(n)
    for k in range(1, n):
        p = lax.rem(me + k, n)
        remote(att_ref.at[p], ra.at[me], a_send.at[p], a_recv.at[me], p).start()
    ra[me] = att_ref[me]
    for k in range(1, n):
        p = lax.rem(me + k, n)
        remote(att_ref.at[p], ra.at[p], a_send.at[p], a_recv.at[p], p).wait_recv()
    slots = ra.shape[0] * ra.shape[1]
    rows[...] = jnp.dot(
        ret_ref[...], ra[...].reshape(slots, ra.shape[2]), preferred_element_type=F32
    ).astype(BF16)

    def core_copy(ch):
        return remote(cs.at[ch], cr.at[ch], c_send.at[ch], c_recv.at[ch], other_c)

    def y_copy(ch):
        return remote(ys.at[ch], yr.at[ch], y_send.at[ch], y_recv.at[ch], other_y)

    def z_copy(ch, zz):
        return remote(
            zs.at[ch, zz], zr.at[ch, z], z_send.at[ch, zz], z_recv.at[ch, z], dev(zz, y, c)
        )

    def z_wait(ch, zz):
        remote(
            zs.at[ch, zz], zr.at[ch, zz], z_send.at[ch, zz], z_recv.at[ch, zz], dev(zz, y, c)
        ).wait_recv()

    def matmul(ch):
        weight_copies[ch].wait()
        step = min(1024, NW)
        for i in range(NW // step):
            off = ch * NW + i * step
            pf[ch, :, i * step : (i + 1) * step] = jnp.dot(
                rows[...], wo[:, off : off + step], preferred_element_type=F32
            )
        cs[ch] = pf[ch, pl.ds(pl.multiple_of((1 - c) * H, H), H), :].astype(BF16)
        core_copy(ch).start()

    def core_step(ch):
        core_copy(ch).wait_recv()
        s1[ch] = pf[ch, pl.ds(pl.multiple_of(c * H, H), H), :] + cr[ch].astype(F32)
        ys[ch] = s1[ch, pl.ds(pl.multiple_of((1 - y) * Q, Q), Q), :].astype(BF16)
        y_copy(ch).start()

    def y_step(ch):
        y_copy(ch).wait_recv()
        s = s1[ch, pl.ds(pl.multiple_of(y * Q, Q), Q), :] + yr[ch].astype(F32)
        for zz in range(Z):
            zf[ch, zz] = s[zz * rl : (zz + 1) * rl]
            zs[ch, zz] = s[zz * rl : (zz + 1) * rl].astype(BF16)
        for k in range(1, Z):
            z_copy(ch, lax.rem(z + k, Z)).start()

    def z_step(ch):
        cols = slice(ch * NW, (ch + 1) * NW)
        total = x_ref[:, cols].astype(F32) + zf[ch, z]
        for k in range(1, Z):
            zz = lax.rem(z + k, Z)
            z_wait(ch, zz)
            total = total + zr[ch, zz].astype(F32)
        out_ref[:, cols] = total.astype(BF16)

    for i in range(NF + 5):
        if i < NF:
            matmul(i)
        if 0 <= i - 1 < NF:
            core_step(i - 1)
        if 0 <= i - 3 < NF:
            y_step(i - 3)
        if 0 <= i - 5 < NF:
            z_step(i - 5)
    for k in range(1, n):
        p = lax.rem(me + k, n)
        remote(att_ref.at[p], ra.at[me], a_send.at[p], a_recv.at[me], p).wait_send()
    for ch in range(NF):
        core_copy(ch).wait_send()
        y_copy(ch).wait_send()
        for k in range(1, Z):
            z_copy(ch, lax.rem(z + k, Z)).wait_send()


def project_out(n, att, ret, x, wo):
    rl, D = x.shape
    NF = 4
    NW = D // NF
    R = n * rl
    Z = n // 4
    vm = pl.BlockSpec(memory_space=pltpu.VMEM)
    hbm = pl.BlockSpec(memory_space=pl.ANY)
    dma = pltpu.SemaphoreType.DMA
    return pl.pallas_call(
        functools.partial(second_kernel, n, NF),
        out_shape=jax.ShapeDtypeStruct((rl, D), BF16),
        in_specs=[vm, vm, vm, hbm],
        out_specs=vm,
        scratch_shapes=[
            pltpu.VMEM(wo.shape, BF16),
            pltpu.VMEM(att.shape, BF16),
            pltpu.VMEM((R, wo.shape[0]), BF16),
            pltpu.VMEM((NF, R, NW), F32),
            pltpu.VMEM((NF, R // 2, NW), BF16),
            pltpu.VMEM((NF, R // 2, NW), BF16),
            pltpu.VMEM((NF, R // 2, NW), F32),
            pltpu.VMEM((NF, R // 4, NW), BF16),
            pltpu.VMEM((NF, R // 4, NW), BF16),
            pltpu.VMEM((NF, Z, rl, NW), F32),
            pltpu.VMEM((NF, Z, rl, NW), BF16),
            pltpu.VMEM((NF, Z, rl, NW), BF16),
            dma((NF,)),
            dma((n,)),
            dma((n,)),
            dma((NF,)),
            dma((NF,)),
            dma((NF,)),
            dma((NF,)),
            dma((NF, Z)),
            dma((NF, Z)),
        ],
        compiler_params=pltpu.CompilerParams(
            collective_id=1, has_side_effects=True, vmem_limit_bytes=60 * 1024 * 1024
        ),
        name="project_out",
    )(att, ret, x, wo)


def attend_slots(probe_vectors, new_kv, keys, values, slot_lengths):
    slots = probe_vectors.shape[0]
    query_heads = probe_vectors.reshape(slots, KV, HEADS // KV, DH)
    key_heads = keys.reshape(slots, CACHE, KV, DH)
    value_heads = values.reshape(slots, CACHE, KV, DH)
    inverse = 1.0 / jnp.sqrt(jnp.float32(DH))
    scores = (
        jnp.einsum("skgd,sjkd->skgj", query_heads, key_heads, preferred_element_type=jnp.float32)
        * inverse
    )
    visible = (jnp.arange(CACHE, dtype=jnp.int32)[None, :] < slot_lengths[:, None])[
        :, None, None, :
    ]
    scores = jnp.where(visible, scores, jnp.float32(-1e30))
    new_keys = new_kv[:, : KV * DH].astype(jnp.float32).reshape(slots, KV, 1, DH)
    new_values = new_kv[:, KV * DH :].astype(jnp.float32).reshape(slots, KV, 1, DH)
    own_score = jnp.sum(query_heads.astype(jnp.float32) * new_keys, axis=-1) * inverse
    highest = jnp.maximum(jnp.max(scores, axis=-1), own_score)
    expo_cache = jnp.where(visible, jnp.exp(scores - highest[..., None]), jnp.float32(0.0))
    expo_new = jnp.exp(own_score - highest)
    denominator = jnp.sum(expo_cache, axis=-1) + expo_new
    weights = (expo_cache / denominator[..., None]).astype(jnp.bfloat16)
    weight_new = (expo_new / denominator).astype(jnp.bfloat16)
    summed = jnp.einsum("skgj,sjkd->skgd", weights, value_heads, preferred_element_type=jnp.float32)
    summed = summed + weight_new.astype(jnp.float32)[..., None] * new_values
    return summed.reshape(slots, HEADS * DH).astype(jnp.bfloat16)


def local(
    remaining_states,
    scaling_factor_vector,
    probe_projection_matrix,
    memory_projection_matrix,
    final_projection_matrix,
    memorized_address_tensor,
    memorized_content_tensor,
    retained_sequence_ids,
    occupied_positions,
):
    n = lax.axis_size("gx")
    me = lax.axis_index("gx")
    slots = memorized_address_tensor.shape[0]
    rl = remaining_states.shape[0]
    R = n * rl
    q_all, kv_all = project_in(
        n,
        remaining_states,
        scaling_factor_vector,
        probe_projection_matrix,
        memory_projection_matrix,
    )
    mine = (
        retained_sequence_ids[None, :]
        == (me * slots + jnp.arange(slots, dtype=jnp.int32))[:, None]
    ).astype(BF16)
    owner_queries = jnp.einsum(
        "sr,drc->sdc", mine, q_all, preferred_element_type=F32
    ).astype(BF16).reshape(slots, -1)
    new_kv = jnp.dot(
        mine, kv_all.reshape(R, -1), preferred_element_type=F32
    ).astype(BF16)
    attended = attend_slots(
        owner_queries,
        new_kv,
        memorized_address_tensor,
        memorized_content_tensor,
        occupied_positions,
    )
    att = jnp.transpose(attended.reshape(slots, n, -1), (1, 0, 2))
    ids = jnp.transpose(
        retained_sequence_ids.reshape(n // 4, 2, 2, rl), (2, 1, 0, 3)
    ).reshape(R)
    ret = (ids[:, None] == jnp.arange(n * slots, dtype=jnp.int32)[None, :]).astype(BF16)
    return project_out(n, att, ret, remaining_states, final_projection_matrix)


def solution(mesh):
    placed = (
        P(("grp", "gx"), None),
        P(),
        P(None, "gx"),
        P("gx", None),
        P("gx", None),
        P(("grp", "gx"), None, None),
        P(("grp", "gx"), None, None),
        P("grp"),
        P(("grp", "gx")),
    )
    return jax.shard_map(
        local, mesh=mesh, in_specs=placed, out_specs=P(("grp", "gx"), None), check_vma=False
    )
```
